32 devices in a mesh: row: 4 (over x, core), col: 8 (over z, y).
Axes of the slice: x: 2, y: 2, z: 4, core: 2. Of those that a mesh axis runs over, the one named last changes fastest.
Arguments:
- picture_embedding_matrix: bfloat16 [2048, 1152], P(('row', 'col')), may hold values from -0.19921875 to 0.19921875
- caption_embedding_matrix: bfloat16 [2048, 1152], P(('row', 'col')), may hold values from -0.19921875 to 0.19921875
- sharpness_scale: float32 [1], replicated, may hold values from 4 to 12
- additive_shift: float32 [1], replicated, may hold values from -4 to -2
Outputs:
- grad_images: float32 [2048, 1152], P(('row', 'col'))
- grad_texts: float32 [2048, 1152], P(('row', 'col'))
- image_loss: float32 [2048], P(('row', 'col'))
The draws below stay inside these ranges and needn't reach their ends.
All inputs are finite; a program needn't handle non-finite values.
Results may differ from the reference program's by a relative error of at most 0.0053.
Values may be sent and summed in bfloat16 or wider, within the bound.
A program may use at most 128 MiB of HBM per device.

```python
import jax
import jax.numpy as jnp
from jax import lax

D = 1152
ROWS_DEV = 64
BATCH = 2048
N_COL = 8


def block_levels(rng, extent, pieces, least, high):
    level, own = 1.0, jax.random.fold_in(rng, 6)
    for position, shards_of in pieces:
        heights = jnp.exp(jax.random.uniform(jax.random.fold_in(own, position), (shards_of,), jnp.float32, least / len(pieces), high / len(pieces)))
        level = level * jnp.repeat(heights, extent[position] // shards_of).reshape([-1 if axis == position else 1 for axis in range(len(extent))])
    return level


def scatter_about(rng, extent, spread, most, split=(), kind=jnp.bfloat16):
    entries = spread * jax.random.normal(rng, extent, jnp.float32)
    if split:
        entries = entries * block_levels(rng, extent, split, -0.22, 0.18)
    return jnp.clip(entries, -most, most).astype(kind)


def setup_inputs(seed: int = 0) -> dict:
    splits = jax.random.split(jax.random.key(seed), 5)
    return {
        "picture_embedding_matrix": scatter_about(splits[0], (BATCH, D), 0.03, 0.19921875, ((0, 32),)),
        "caption_embedding_matrix": scatter_about(splits[1], (BATCH, D), 0.03, 0.19921875, ((0, 32),)),
        "sharpness_scale": jnp.clip(jax.random.uniform(splits[2], (1,), jnp.float32, 4.0, 12.0), 4.0, 12.0),
        "additive_shift": jnp.clip(jax.random.uniform(splits[3], (1,), jnp.float32, -4.0, -2.0), -4.0, -2.0),
    }


EPS = 1e-06

def normalize(feats):
    values = feats.astype(jnp.float32)
    inverse = lax.rsqrt(lax.optimization_barrier(jnp.sum(values * values, axis=-1, keepdims=True)) + EPS)
    return (values * inverse, inverse)

def back_norm(grad, unit, inverse):
    return inverse * (grad - unit * lax.optimization_barrier(jnp.sum(unit * grad, axis=-1, keepdims=True)))

def reference(picture_embedding_matrix, caption_embedding_matrix, sharpness_scale, additive_shift):
    img_f, img_inv = normalize(picture_embedding_matrix)
    txt_f, txt_inv = normalize(caption_embedding_matrix)
    img_b = img_f.astype(jnp.bfloat16)
    caption_segment = txt_f.astype(jnp.bfloat16)
    block = ROWS_DEV * N_COL
    blocks = BATCH // block
    columns = jnp.arange(BATCH, dtype=jnp.int32)

    def step(acc, index):
        start = (index * block).astype(jnp.int32)
        sample_total = lax.dynamic_slice_in_dim(img_b, start, block, 0)
        similarity_matrix = jnp.dot(sample_total, caption_segment.T, preferred_element_type=jnp.float32) * sharpness_scale[0] + additive_shift[0]
        ids = start + jnp.arange(block, dtype=jnp.int32)
        match_sign = ids[:, None] == columns[None, :]
        label = jnp.where(match_sign, jnp.float32(1.0), jnp.float32(-1.0))
        sigmoid_loss = lax.optimization_barrier(jnp.sum(jnp.log1p(jnp.exp(-label * similarity_matrix)), axis=1))
        logistic_weight = (sharpness_scale[0] * (jax.nn.sigmoid(similarity_matrix) - match_sign.astype(jnp.float32))).astype(jnp.bfloat16)
        g_rows = jnp.dot(logistic_weight, caption_segment, preferred_element_type=jnp.float32)
        acc = acc + lax.dot_general(logistic_weight, sample_total, (((0,), (0,)), ((), ())), preferred_element_type=jnp.float32)
        return (acc, (g_rows, sigmoid_loss))
    start_acc = jnp.zeros((BATCH, D), jnp.float32)
    g_txt, (g_img, sigmoid_loss) = lax.scan(step, start_acc, jnp.arange(blocks, dtype=jnp.int32))
    g_img = g_img.reshape(BATCH, D)
    sigmoid_loss = sigmoid_loss.reshape(BATCH)
    return (back_norm(g_img, img_f, img_inv), back_norm(g_txt, txt_f, txt_inv), sigmoid_loss)
```

```python
import functools

import jax
import jax.numpy as jnp
from jax import lax
from jax.experimental import pallas as pl
from jax.experimental.pallas import tpu as pltpu
from jax.sharding import PartitionSpec as P

EPS = 1e-06
MESH = pl.DeviceIdType.MESH
CORE = ("row", 0)
TILE = 256


def bits_of(n):
    return n.bit_length() - 1


def groups(n_row, n_col):
    row_bits, col_bits = bits_of(n_row), bits_of(n_col)
    take = min(max((row_bits + col_bits + 1) // 2 - row_bits, 0), col_bits)
    choice = [b for b in range(1, col_bits)] + [0] * (col_bits > 0)
    mine, rest = choice[:take], choice[take:]
    images = [("col", b) for b in sorted(mine, reverse=True)]
    images += [("row", b) for b in reversed(range(1, row_bits))]
    texts = [("col", b) for b in sorted(rest, reverse=True)]
    return images, texts


def flip(index, bit):
    step = 2**bit
    return index + step * (1 - 2 * lax.rem(lax.div(index, step), 2))


def across(axis, bit):
    at = {"row": lax.axis_index("row"), "col": lax.axis_index("col")}
    at[axis] = flip(at[axis], bit)
    return (at["row"], at["col"])


def top(slot):
    return slot.bit_length() - 1


def pieces_of(rows):
    quarter = rows // 4
    return [(0, quarter), (quarter, rows - 2 * quarter), (rows - quarter, quarter)]


def inverse_norm(values):
    return lax.rsqrt(jnp.sum(values * values, axis=-1, keepdims=True) + EPS)


def tiles(count, body):
    if count <= 4:
        for t in range(count):
            body(t)
    else:
        lax.fori_loop(0, count, lambda t, _: (body(t), 0)[1], 0)


def kernel(
    dims,
    img_hbm,
    txt_hbm,
    scale_ref,
    shift_ref,
    gi_ref,
    gt_ref,
    loss_ref,
    raw_img,
    raw_txt,
    unit_img,
    unit_txt,
    coef_img,
    coef_txt,
    acc_img,
    acc_txt,
    out_img,
    out_txt,
    in_img,
    in_txt,
    loss_lanes,
    loss_acc,
    loss_out,
    loss_in,
    load,
    sends,
    gr_img,
    gr_txt,
    cr_img,
    cr_txt,
    sr_img,
    sr_txt,
    lr,
):
    rows, width = img_hbm.shape
    cuts = pieces_of(rows)
    n_cuts = len(cuts)
    other = {"i": "t", "t": "i"}
    size = {g: 2 ** len(dims[g]) for g in "it"}
    raw = {"i": raw_img, "t": raw_txt}
    unit = {"i": unit_img, "t": unit_txt}
    coef = {"i": coef_img, "t": coef_txt}
    acc = {"i": acc_img, "t": acc_txt}
    out = {"i": out_img, "t": out_txt}
    into = {"i": in_img, "t": in_txt}
    g_recv = {"i": gr_img, "t": gr_txt}
    c_recv = {"i": cr_img, "t": cr_txt}
    s_recv = {"i": sr_img, "t": sr_txt}
    g_send = {"i": sends.at[0], "t": sends.at[1]}
    s_send = {"i": sends.at[2], "t": sends.at[3]}
    l_send = sends.at[4]

    peers = [across(*CORE)] + [across(*d) for g in "it" for d in dims[g]]
    barrier = pltpu.get_barrier_semaphore()
    for peer in peers:
        pl.semaphore_signal(barrier, inc=1, device_id=peer, device_id_type=MESH)
    loads = [
        pltpu.make_async_copy(source, target.at[0], load.at[n])
        for n, (source, target) in enumerate([(txt_hbm, raw_txt), (img_hbm, raw_img)])
    ]
    for copy in loads:
        copy.start()
    for copy in loads:
        copy.wait()
    pl.semaphore_wait(barrier, len(peers))

    gather = {}

    def spread(g, slot, j, p):
        to = slot | 1 << j
        piece = pl.ds(*cuts[p])
        copy = pltpu.make_async_remote_copy(
            src_ref=raw[g].at[slot, piece],
            dst_ref=raw[g].at[to, piece],
            send_sem=g_send[g],
            recv_sem=g_recv[g].at[to * n_cuts + p],
            device_id=across(*dims[g][j]),
            device_id_type=MESH,
        )
        copy.start()
        gather[g, to, p] = copy

    def share(g, slot, piece):
        return pltpu.make_async_remote_copy(
            src_ref=raw[g].at[slot, piece],
            dst_ref=raw[g].at[size[g] + slot, piece],
            send_sem=g_send[g],
            recv_sem=c_recv[g].at[slot],
            device_id=across(*CORE),
            device_id_type=MESH,
        )

    levels = max(len(d) for d in dims.values())
    for p in range(n_cuts):
        for j in range(levels):
            for g in "ti":
                if j < len(dims[g]):
                    spread(g, 0, j, p)
    for g in "ti":
        share(g, 0, pl.ds(0, rows)).start()

    def normalize(g, slot, core):
        values = raw[g][core * size[g] + slot].astype(jnp.float32)
        unit[g][slot, core] = (values * inverse_norm(values)).astype(jnp.bfloat16)

    def partner(g, slot):
        share(g, slot, pl.ds(0, rows)).wait_recv()
        normalize(g, slot, 1)

    for g in "ti":
        normalize(g, 0, 0)
    for g in "ti":
        partner(g, 0)
    for level in range(1, levels + 1):
        slots = [
            (g, s)
            for s in reversed(range(1, max(size.values())))
            for g in "ti"
            if s < size[g] and s.bit_count() == level
        ]
        for p in range(n_cuts):
            for g, s in slots:
                gather[g, s, p].wait_recv()
                for j in range(top(s) + 1, len(dims[g])):
                    spread(g, s, j, p)
                share(g, s, pl.ds(*cuts[p])).start()
                if p == n_cuts - 1:
                    normalize(g, s, 0)
        for g, s in slots:
            partner(g, s)

    scale, shift = scale_ref[0], shift_ref[0]
    n_mine = {g: size[g] * rows for g in "it"}

    def logits(g, t):
        o = other[g]
        take_r = min(TILE // rows, size[g])
        take_c = min(TILE // rows // 2, size[o])
        n_r, n_c = take_r * rows, take_c * 2 * rows
        steps = size[o] // take_c
        if isinstance(t, int):
            r, c = t // steps * take_r, t % steps * take_c
            at_r, at_c = r * rows, c * 2 * rows
        else:
            r, c = lax.div(t, steps) * take_r, lax.rem(t, steps) * take_c
            at_r = pl.multiple_of(r * rows, n_r)
            at_c = pl.multiple_of(c * 2 * rows, n_c)
        left = unit[g][pl.ds(r, take_r), 0].reshape(n_r, width)
        right = unit[o][pl.ds(c, take_c)].reshape(n_c, width)
        value = lax.dot_general(
            left, right, (((1,), (1,)), ((), ())), preferred_element_type=jnp.float32
        )
        value = value * scale + shift
        weight = scale
        if not isinstance(t, int) or t == 0:
            a = lax.broadcasted_iota(jnp.int32, value.shape, 0) + at_r
            b = lax.broadcasted_iota(jnp.int32, value.shape, 1) + at_c
            match = (a == b) & (a < rows)
            value = jnp.where(match, -value, value)
            weight = jnp.where(match, -scale, scale)
        e = jnp.exp(value)
        coef[g][pl.ds(at_r, n_r), pl.ds(at_c, n_c)] = (weight * (e / (1.0 + e))).astype(
            jnp.bfloat16
        )
        if g == "i":
            terms = jnp.log1p(e)
            fold = terms[:, :128]
            for k in range(1, n_c // 128):
                fold = fold + terms[:, k * 128 : (k + 1) * 128]
            if isinstance(t, int) and t % steps == 0:
                loss_lanes[pl.ds(at_r, n_r), :] = fold
            else:
                loss_lanes[pl.ds(at_r, n_r), :] += fold

    def all_logits(g):
        o = other[g]
        count = -(-size[g] // (TILE // rows)) * -(-size[o] * 2 // (TILE // rows))
        if g == "i" and count > 4:
            loss_lanes[...] = jnp.zeros_like(loss_lanes)
        tiles(count, functools.partial(logits, g))

    scatter = {}

    def pass_on(g, s, p):
        piece = pl.ds(*cuts[p])
        copy = pltpu.make_async_remote_copy(
            src_ref=out[g].at[s, piece],
            dst_ref=into[g].at[s, piece],
            send_sem=s_send[g],
            recv_sem=s_recv[g].at[s * n_cuts + p],
            device_id=across(*dims[g][top(s)]),
            device_id_type=MESH,
        )
        copy.start()
        scatter[g, s, p] = copy

    def grads(g, upper):
        half = size[g] // 2
        base = half if upper else 0
        step = min(half, TILE // rows)
        o = other[g]

        def body(t):
            first = base + t * step
            here = first * rows
            if not isinstance(first, int):
                here = pl.multiple_of(here, step * rows)
            value = jnp.dot(
                coef[g][pl.ds(here, step * rows), :],
                unit[o][...].reshape(2 * n_mine[o], width),
                preferred_element_type=jnp.float32,
            ).reshape(step, rows, width)
            if upper:
                out[g][pl.ds(first, step)] = value.astype(jnp.bfloat16)
            else:
                acc[g][pl.ds(first, step)] = value

        tiles(half // step, body)
        if upper:
            for s in reversed(range(half, size[g])):
                for p in range(n_cuts):
                    pass_on(g, s, p)

    all_logits("t")
    grads("t", True)
    all_logits("i")
    grads("i", True)

    losses = {}

    def loss_on(s, value):
        loss_out[s] = value
        copy = pltpu.make_async_remote_copy(
            src_ref=loss_out.at[s],
            dst_ref=loss_in.at[s],
            send_sem=l_send,
            recv_sem=lr.at[s],
            device_id=across(*dims["i"][top(s)]),
            device_id_type=MESH,
        )
        copy.start()
        losses[s] = copy

    def loss_total(k):
        value = loss_acc[:, k * rows : (k + 1) * rows]
        for j in reversed(range(top(k) + 1 if k else 0, len(dims["i"]))):
            losses[k | 1 << j].wait_recv()
            value = value + loss_in[k | 1 << j]
        return value

    loss_acc[...] = jnp.sum(loss_lanes[...].T, axis=0, keepdims=True)
    for s in reversed(range(size["i"] // 2, size["i"])):
        loss_on(s, loss_acc[:, s * rows : (s + 1) * rows])
    grads("t", False)
    grads("i", False)

    def total(g, k, p):
        piece = pl.ds(*cuts[p])
        value = acc[g][k, piece]
        for j in reversed(range(top(k) + 1 if k else 0, len(dims[g]))):
            scatter[g, k | 1 << j, p].wait_recv()
            value = value + into[g][k | 1 << j, piece].astype(jnp.float32)
        return value

    order = sorted(
        [(k.bit_length() - len(dims[g]), g, k) for g in "it" for k in range(1, size[g] // 2)],
        key=lambda item: (-item[0], item[1] != "t", -item[2]),
    )
    for p in range(n_cuts):
        for _, g, k in order:
            out[g][k, pl.ds(*cuts[p])] = total(g, k, p).astype(jnp.bfloat16)
            pass_on(g, k, p)
    for k in reversed(range(1, size["i"] // 2)):
        loss_on(k, loss_total(k))

    for p in range(n_cuts):
        for g, result in (("t", gt_ref), ("i", gi_ref)):
            piece = pl.ds(*cuts[p])
            grad = total(g, 0, p)
            values = raw[g][0, piece].astype(jnp.float32)
            inverse = inverse_norm(values)
            unit_row = values * inverse
            along = jnp.sum(unit_row * grad, axis=-1, keepdims=True)
            result[piece, :] = inverse * (grad - unit_row * along)
    loss_ref[...] = loss_total(0)

    def drain(ref, sem):
        pltpu.make_async_remote_copy(
            src_ref=ref,
            dst_ref=ref,
            send_sem=sem,
            recv_sem=sem,
            device_id=across(*CORE),
            device_id_type=MESH,
        ).wait_send()

    for g in "it":
        drain(raw[g].at[pl.ds(0, 2 * size[g] - 1)], g_send[g])
        drain(out[g].at[pl.ds(1, size[g] - 1)], s_send[g])
    drain(loss_out.at[pl.ds(1, size["i"] - 1)], l_send)


def hand_out(gi_from, gt_from, loss_from, gi_ref, gt_ref, loss_ref, sems):
    pairs = ((gi_from, gi_ref), (gt_from, gt_ref), (loss_from, loss_ref))
    copies = [pltpu.make_async_copy(a, b, sems.at[n]) for n, (a, b) in enumerate(pairs)]
    for copy in copies:
        copy.start()
    for copy in copies:
        copy.wait()


def on_device(n_row, n_col, images, texts, scale, shift):
    rows, width = images.shape
    dims = dict(zip("it", groups(n_row, n_col)))
    a, b = 2 ** len(dims["i"]), 2 ** len(dims["t"])
    n_cuts = len(pieces_of(rows))
    vmem = pl.BlockSpec(memory_space=pltpu.VMEM)
    smem = pl.BlockSpec(memory_space=pltpu.SMEM)
    hbm = pl.BlockSpec(memory_space=pl.ANY)
    f32, bf16 = jnp.float32, jnp.bfloat16
    dma = pltpu.SemaphoreType.DMA
    sums = pl.pallas_call(
        functools.partial(kernel, dims),
        out_shape=(
            pltpu.VMEM((rows, width), f32),
            pltpu.VMEM((rows, width), f32),
            pltpu.VMEM((1, rows), f32),
        ),
        in_specs=[hbm, hbm, smem, smem],
        out_specs=(vmem, vmem, vmem),
        scratch_shapes=[
            pltpu.VMEM((2 * a, rows, width), bf16),
            pltpu.VMEM((2 * b, rows, width), bf16),
            pltpu.VMEM((a, 2, rows, width), bf16),
            pltpu.VMEM((b, 2, rows, width), bf16),
            pltpu.VMEM((a * rows, 2 * b * rows), bf16),
            pltpu.VMEM((b * rows, 2 * a * rows), bf16),
            pltpu.VMEM((a // 2, rows, width), f32),
            pltpu.VMEM((b // 2, rows, width), f32),
            pltpu.VMEM((a, rows, width), bf16),
            pltpu.VMEM((b, rows, width), bf16),
            pltpu.VMEM((a, rows, width), bf16),
            pltpu.VMEM((b, rows, width), bf16),
            pltpu.VMEM((a * rows, 128), f32),
            pltpu.VMEM((1, a * rows), f32),
            pltpu.VMEM((a, 1, rows), f32),
            pltpu.VMEM((a, 1, rows), f32),
            dma((2,)),
            dma((5,)),
            dma((a * n_cuts,)),
            dma((b * n_cuts,)),
            dma((a,)),
            dma((b,)),
            dma((a * n_cuts,)),
            dma((b * n_cuts,)),
            dma((a,)),
        ],
        compiler_params=pltpu.CompilerParams(collective_id=0, has_side_effects=True),
    )(*[pltpu.with_memory_space_constraint(x, pltpu.HBM) for x in (images, texts)], scale, shift)
    gi, gt, loss = pl.pallas_call(
        hand_out,
        out_shape=(
            jax.ShapeDtypeStruct((rows, width), f32),
            jax.ShapeDtypeStruct((rows, width), f32),
            jax.ShapeDtypeStruct((1, rows), f32),
        ),
        in_specs=[hbm] * 3,
        out_specs=(hbm, hbm, hbm),
        scratch_shapes=[pltpu.SemaphoreType.DMA((3,))],
    )(*[pltpu.with_memory_space_constraint(x, pltpu.VMEM) for x in sums])
    return gi, gt, loss.reshape(rows)


def solution(mesh):
    placed = (P(("row", "col"), None), P(("row", "col"), None), P(), P())
    return jax.shard_map(
        functools.partial(on_device, mesh.shape["row"], mesh.shape["col"]),
        mesh=mesh,
        in_specs=placed,
        out_specs=(P(("row", "col"), None), P(("row", "col"), None), P(("row", "col"))),
        check_vma=False,
    )
```

```python
import functools
import heapq

import jax
import jax.numpy as jnp
from jax import lax
from jax.experimental import pallas as pl
from jax.experimental.pallas import tpu as pltpu
from jax.sharding import PartitionSpec as P

EPS = 1e-06
MESH = pl.DeviceIdType.MESH
CORE = ("row", 0)
TILE = 256


def bits_of(n):
    return n.bit_length() - 1


def groups(n_row, n_col):
    row_bits, col_bits = bits_of(n_row), bits_of(n_col)
    take = min(max((row_bits + col_bits + 1) // 2 - row_bits, 0), col_bits)
    choice = [b for b in range(1, col_bits)] + [0] * (col_bits > 0)
    mine, rest = choice[:take], choice[take:]
    images = [("row", b) for b in range(1, row_bits)] + [("col", b) for b in sorted(mine)]
    texts = [("col", b) for b in sorted(rest)]
    return images, texts


def flip(index, bit):
    step = 2**bit
    return index + step * (1 - 2 * lax.rem(lax.div(index, step), 2))


def across(axis, bit):
    at = {"row": lax.axis_index("row"), "col": lax.axis_index("col")}
    at[axis] = flip(at[axis], bit)
    return (at["row"], at["col"])


def cuts_of(rows):
    quarter = rows // 4
    return [(p * quarter, quarter) for p in range(4)]


def order_of(n_dims, p):
    return list(range(n_dims)) if p == 3 else list(reversed(range(n_dims)))


def last_bit(slot, order):
    return [j for j in order if slot >> j & 1][-1]


def later(slot, order):
    return order[order.index(last_bit(slot, order)) + 1 :] if slot else order


def expected(nodes):
    ready = [(0, rank, key) for key, (_, _, deps, rank) in nodes.items() if not deps]
    heapq.heapify(ready)
    users = {}
    for key, (_, _, deps, _) in nodes.items():
        for dep in deps:
            users.setdefault(dep, []).append(key)
    free, arrival = {}, {}
    while ready:
        at, _, key = heapq.heappop(ready)
        link, latency, _, _ = nodes[key]
        free[link] = max(at, free.get(link, 0)) + (1 if link else 0)
        arrival[key] = max(at, free[link]) + latency
        for user in users.get(key, []):
            _, _, deps, rank = nodes[user]
            if all(d in arrival for d in deps):
                heapq.heappush(ready, (max(arrival[d] for d in deps), rank, user))
    return arrival


def link_of(dim):
    axis, bit = dim
    return (axis, axis == "col" and bit > 0), 2 + (axis == "col" and bit > 1)


def inverse_norm(values):
    return lax.rsqrt(jnp.sum(values * values, axis=-1, keepdims=True) + EPS)


def tiles(count, body):
    if count <= 4:
        for t in range(count):
            body(t)
    else:
        lax.fori_loop(0, count, lambda t, _: (body(t), 0)[1], 0)


def kernel(
    dims,
    img_hbm,
    txt_hbm,
    scale_ref,
    shift_ref,
    gi_ref,
    gt_ref,
    loss_ref,
    raw_img,
    raw_txt,
    unit_img,
    unit_txt,
    coef_img,
    coef_txt,
    acc_img,
    acc_txt,
    out_img,
    out_txt,
    in_img,
    in_txt,
    loss_lanes,
    loss_acc,
    loss_out,
    loss_in,
    load,
    sends,
    gr_img,
    gr_txt,
    cr_img,
    cr_txt,
    sr_img,
    sr_txt,
    lr,
):
    rows, width = img_hbm.shape
    cuts = cuts_of(rows)
    n_cuts = len(cuts)
    other = {"i": "t", "t": "i"}
    size = {g: 2 ** len(dims[g]) for g in "it"}
    order = {g: [order_of(len(dims[g]), p) for p in range(n_cuts)] for g in "it"}
    raw = {"i": raw_img, "t": raw_txt}
    unit = {"i": unit_img, "t": unit_txt}
    coef = {"i": coef_img, "t": coef_txt}
    acc = {"i": acc_img, "t": acc_txt}
    out = {"i": out_img, "t": out_txt}
    into = {"i": in_img, "t": in_txt}
    g_recv = {"i": gr_img, "t": gr_txt}
    c_recv = {"i": cr_img, "t": cr_txt}
    s_recv = {"i": sr_img, "t": sr_txt}
    g_send = {"i": sends.at[0], "t": sends.at[1]}
    c_send = {"i": sends.at[2], "t": sends.at[3]}
    s_send = {"i": sends.at[4], "t": sends.at[5]}
    l_send = sends.at[6]

    peers = [across(*CORE)] + [across(*d) for g in "it" for d in dims[g]]
    barrier = pltpu.get_barrier_semaphore()
    for peer in peers:
        pl.semaphore_signal(barrier, inc=1, device_id=peer, device_id_type=MESH)
    loads = [
        pltpu.make_async_copy(source, target.at[0], load.at[n])
        for n, (source, target) in enumerate([(txt_hbm, raw_txt), (img_hbm, raw_img)])
    ]
    for copy in loads:
        copy.start()
    for copy in loads:
        copy.wait()
    pl.semaphore_wait(barrier, len(peers))

    gather = {}
    keys = [(g, s, p) for g in "ti" for s in range(1, size[g]) for p in range(n_cuts)]

    def spread(g, to, p):
        j = last_bit(to, order[g][p])
        piece = pl.ds(*cuts[p])
        copy = pltpu.make_async_remote_copy(
            src_ref=raw[g].at[to ^ 1 << j, piece],
            dst_ref=raw[g].at[to, piece],
            send_sem=g_send[g],
            recv_sem=g_recv[g].at[(to - 1) * n_cuts + p],
            device_id=across(*dims[g][j]),
            device_id_type=MESH,
        )
        copy.start()
        gather[g, to, p] = copy

    def share(g, slot, piece):
        return pltpu.make_async_remote_copy(
            src_ref=unit[g].at[slot, 0, piece],
            dst_ref=unit[g].at[slot, 1, piece],
            send_sem=c_send[g],
            recv_sem=c_recv[g].at[slot],
            device_id=across(*CORE),
            device_id_type=MESH,
        )

    def normalize(g, slot, piece):
        values = raw[g][slot, piece].astype(jnp.float32)
        unit[g][slot, 0, piece] = (values * inverse_norm(values)).astype(jnp.bfloat16)
        share(g, slot, piece).start()

    nodes = {}
    for g, to, p in keys:
        j = last_bit(to, order[g][p])
        rest = to ^ 1 << j
        rank = (order[g][p].index(j), p, g == "i")
        nodes[g, to, p] = (*link_of(dims[g][j]), [(g, rest, p)] if rest else [], rank)
    arrival = expected(nodes)
    for g, to, p in sorted(keys, key=lambda key: nodes[key][3]):
        if to.bit_count() == 1:
            spread(g, to, p)
    for g in "ti":
        normalize(g, 0, pl.ds(0, rows))

    def partner(slot):
        for g in "it":
            if slot < size[g]:
                share(g, slot, pl.ds(0, rows)).wait_recv()

    scale, shift = scale_ref[0], shift_ref[0]
    n_mine = {g: size[g] * rows for g in "it"}

    def tile(g, r, take_r, c, take_c):
        o = other[g]
        n_r, n_c = take_r * rows, take_c * 2 * rows
        at_r, at_c = r * rows, c * 2 * rows
        fixed = isinstance(r, int)
        if not fixed:
            at_r, at_c = pl.multiple_of(at_r, n_r), pl.multiple_of(at_c, n_c)
        left = unit[g][pl.ds(r, take_r), 0].reshape(n_r, width)
        right = unit[o][pl.ds(c, take_c)].reshape(n_c, width)
        value = lax.dot_general(
            left, right, (((1,), (1,)), ((), ())), preferred_element_type=jnp.float32
        )
        value = value * scale + shift
        weight = scale
        if not fixed or (r == 0 and c == 0):
            a = lax.broadcasted_iota(jnp.int32, value.shape, 0) + at_r
            b = lax.broadcasted_iota(jnp.int32, value.shape, 1) + at_c
            match = (a == b) & (a < rows)
            value = jnp.where(match, -value, value)
            weight = jnp.where(match, -scale, scale)
        e = jnp.exp(value)
        here = pl.ds(at_r, n_r)
        coef[g][here, pl.ds(at_c, n_c)] = (weight * (e / (1.0 + e))).astype(jnp.bfloat16)
        if g == "i":
            terms = jnp.log1p(e)
            fold = terms[:, :128]
            for k in range(1, n_c // 128):
                fold = fold + terms[:, k * 128 : (k + 1) * 128]
            if fixed and c == 0:
                loss_lanes[here, :] = fold
            else:
                loss_lanes[here, :] += fold

    def all_tiles(g):
        take_r, take_c = min(TILE // rows, size[g]), min(TILE // rows // 2, size[other[g]])
        n_c = size[other[g]] // take_c
        if g == "i":
            loss_lanes[...] = jnp.zeros_like(loss_lanes)
        lax.fori_loop(
            0,
            size[g] // take_r * n_c,
            lambda t, _: (
                tile(g, lax.div(t, n_c) * take_r, take_r, lax.rem(t, n_c) * take_c, take_c),
                0,
            )[1],
            0,
        )

    stream = size["i"] == size["t"] == 4
    steps = {}
    if stream:
        steps[1, True] = [("t", 0, 2, 0, 2), ("i", 0, 2, 0, 2)]
        steps[2, True] = [(g, *at) for g in "ti" for at in ((2, 1, 0, 3), (0, 2, 2, 1))]
        steps[3, False] = [(g, 3, 1, 0, 3) for g in "ti"]
        steps[3, True] = [(g, 0, 4, 3, 1) for g in "ti"]
    left = {s: sum(key[1] == s for key in keys) for s in range(1, max(size.values()))}
    waiting = [0]

    def partners():
        for s in waiting:
            partner(s)
            for args in steps.get((s, True), []):
                tile(*args)
        waiting.clear()

    for g, s, p in sorted(keys, key=lambda key: (arrival[key], nodes[key][3])):
        gather[g, s, p].wait_recv()
        for j in later(s, order[g][p]):
            spread(g, s | 1 << j, p)
        normalize(g, s, pl.ds(*cuts[p]))
        left[s] -= 1
        if left[s] == 0:
            partners()
            for args in steps.get((s, False), []):
                tile(*args)
            waiting.append(s)
    partners()
    if not stream:
        all_tiles("t")
        all_tiles("i")

    scatter = {}

    def pass_on(g, s, p):
        piece = pl.ds(*cuts[p])
        copy = pltpu.make_async_remote_copy(
            src_ref=out[g].at[s, piece],
            dst_ref=into[g].at[s, piece],
            send_sem=s_send[g],
            recv_sem=s_recv[g].at[(s - 1) * n_cuts + p],
            device_id=across(*dims[g][last_bit(s, order[g][p])]),
            device_id_type=MESH,
        )
        copy.start()
        scatter[g, s, p] = copy

    def at_once(g, s, p):
        return s > 0 and not later(s, order[g][p])

    def grads(g, first, count):
        o = other[g]
        step = min(count, TILE // rows)

        def body(t):
            slot = first + t * step
            here = slot * rows
            if not isinstance(slot, int):
                here = pl.multiple_of(here, step * rows)
            value = jnp.dot(
                coef[g][pl.ds(here, step * rows), :],
                unit[o][...].reshape(2 * size[o] * rows, width),
                preferred_element_type=jnp.float32,
            ).reshape(step, rows, width)
            if not isinstance(slot, int):
                acc[g][pl.ds(slot, step)] = value
                out[g][pl.ds(slot, step)] = value.astype(jnp.bfloat16)
                return
            for k in range(step):
                for p, (start, length) in enumerate(cuts):
                    piece = pl.ds(start, length)
                    part = value[k, start : start + length]
                    if at_once(g, slot + k, p):
                        out[g][slot + k, piece] = part.astype(jnp.bfloat16)
                    else:
                        acc[g][slot + k, piece] = part

        tiles(count // step, body)
        for s in reversed(range(first, first + count)):
            for p in range(n_cuts):
                if at_once(g, s, p):
                    pass_on(g, s, p)

    losses = {}
    l_order = order["i"][0]

    def loss_on(s, value):
        loss_out[s] = value
        copy = pltpu.make_async_remote_copy(
            src_ref=loss_out.at[s],
            dst_ref=loss_in.at[s],
            send_sem=l_send,
            recv_sem=lr.at[s - 1],
            device_id=across(*dims["i"][last_bit(s, l_order)]),
            device_id_type=MESH,
        )
        copy.start()
        losses[s] = copy

    def loss_total(k):
        value = loss_acc[:, k * rows : (k + 1) * rows]
        for j in reversed(later(k, l_order)):
            losses[k | 1 << j].wait_recv()
            value = value + loss_in[k | 1 << j]
        return value

    l_later = sorted(
        range(1, size["i"]), key=lambda s: (-l_order.index(last_bit(s, l_order)), -s)
    )
    grads("t", size["t"] // 2, size["t"] // 2)
    loss_acc[...] = jnp.sum(loss_lanes[...].T, axis=0, keepdims=True)
    for s in l_later:
        if not later(s, l_order):
            loss_on(s, loss_acc[:, s * rows : (s + 1) * rows])
    grads("i", size["i"] // 2, size["i"] // 2)
    grads("t", 0, size["t"] // 2)
    grads("i", 0, size["i"] // 2)

    def total(g, k, p):
        piece = pl.ds(*cuts[p])
        value = acc[g][k, piece]
        for j in reversed(later(k, order[g][p])):
            scatter[g, k | 1 << j, p].wait_recv()
            value = value + into[g][k | 1 << j, piece].astype(jnp.float32)
        return value

    nodes = {}
    for g, s, p in keys + [(g, 0, p) for g in "ti" for p in range(n_cuts)]:
        deps = [(g, s | 1 << j, p) for j in later(s, order[g][p])]
        link = link_of(dims[g][last_bit(s, order[g][p])]) if s else (None, 0)
        nodes[g, s, p] = (*link, deps, (-s, p, g == "i"))
    arrival = expected(nodes)
    due = {
        key: (max(arrival[d] for d in deps), rank)
        for key, (_, _, deps, rank) in nodes.items()
        if deps
    }
    result = {"i": gi_ref, "t": gt_ref}
    for g, k, p in sorted(due, key=due.get):
        piece = pl.ds(*cuts[p])
        if k:
            out[g][k, piece] = total(g, k, p).astype(jnp.bfloat16)
            pass_on(g, k, p)
            continue
        if l_later:
            for s in l_later:
                if later(s, l_order):
                    loss_on(s, loss_total(s))
            l_later.clear()
        grad = total(g, 0, p)
        values = raw[g][0, piece].astype(jnp.float32)
        inverse = inverse_norm(values)
        along = jnp.sum(values * grad, axis=-1, keepdims=True)
        result[g][piece, :] = inverse * (grad - values * (inverse * inverse * along))
    loss_ref[...] = loss_total(0)

    def drain(ref, sem):
        pltpu.make_async_remote_copy(
            src_ref=ref,
            dst_ref=ref,
            send_sem=sem,
            recv_sem=sem,
            device_id=across(*CORE),
            device_id_type=MESH,
        ).wait_send()

    for g in "it":
        drain(raw[g].at[pl.ds(1, size[g] - 1)], g_send[g])
        drain(unit[g].at[pl.ds(0, size[g]), 0], c_send[g])
        drain(out[g].at[pl.ds(1, size[g] - 1)], s_send[g])
    drain(loss_out.at[pl.ds(1, size["i"] - 1)], l_send)


def hand_out(gi_from, gt_from, loss_from, gi_ref, gt_ref, loss_ref, sems):
    pairs = ((gi_from, gi_ref), (gt_from, gt_ref), (loss_from, loss_ref))
    copies = [pltpu.make_async_copy(a, b, sems.at[n]) for n, (a, b) in enumerate(pairs)]
    for copy in copies:
        copy.start()
    for copy in copies:
        copy.wait()


def on_device(n_row, n_col, images, texts, scale, shift):
    rows, width = images.shape
    dims = dict(zip("it", groups(n_row, n_col)))
    a, b = 2 ** len(dims["i"]), 2 ** len(dims["t"])
    n_cuts = len(cuts_of(rows))
    vmem = pl.BlockSpec(memory_space=pltpu.VMEM)
    smem = pl.BlockSpec(memory_space=pltpu.SMEM)
    hbm = pl.BlockSpec(memory_space=pl.ANY)
    f32, bf16 = jnp.float32, jnp.bfloat16
    dma = pltpu.SemaphoreType.DMA
    sums = pl.pallas_call(
        functools.partial(kernel, dims),
        out_shape=(
            pltpu.VMEM((rows, width), f32),
            pltpu.VMEM((rows, width), f32),
            pltpu.VMEM((1, rows), f32),
        ),
        in_specs=[hbm, hbm, smem, smem],
        out_specs=(vmem, vmem, vmem),
        scratch_shapes=[
            pltpu.VMEM((a, rows, width), bf16),
            pltpu.VMEM((b, rows, width), bf16),
            pltpu.VMEM((a, 2, rows, width), bf16),
            pltpu.VMEM((b, 2, rows, width), bf16),
            pltpu.VMEM((a * rows, 2 * b * rows), bf16),
            pltpu.VMEM((b * rows, 2 * a * rows), bf16),
            pltpu.VMEM((a, rows, width), f32),
            pltpu.VMEM((b, rows, width), f32),
            pltpu.VMEM((a, rows, width), bf16),
            pltpu.VMEM((b, rows, width), bf16),
            pltpu.VMEM((a, rows, width), bf16),
            pltpu.VMEM((b, rows, width), bf16),
            pltpu.VMEM((a * rows, 128), f32),
            pltpu.VMEM((1, a * rows), f32),
            pltpu.VMEM((a, 1, rows), f32),
            pltpu.VMEM((a, 1, rows), f32),
            dma((2,)),
            dma((7,)),
            dma(((a - 1) * n_cuts,)),
            dma(((b - 1) * n_cuts,)),
            dma((a,)),
            dma((b,)),
            dma(((a - 1) * n_cuts,)),
            dma(((b - 1) * n_cuts,)),
            dma((a - 1,)),
        ],
        compiler_params=pltpu.CompilerParams(collective_id=0, has_side_effects=True),
    )(*[pltpu.with_memory_space_constraint(x, pltpu.HBM) for x in (images, texts)], scale, shift)
    gi, gt, loss = pl.pallas_call(
        hand_out,
        out_shape=(
            jax.ShapeDtypeStruct((rows, width), f32),
            jax.ShapeDtypeStruct((rows, width), f32),
            jax.ShapeDtypeStruct((1, rows), f32),
        ),
        in_specs=[hbm] * 3,
        out_specs=(hbm, hbm, hbm),
        scratch_shapes=[pltpu.SemaphoreType.DMA((3,))],
    )(*[pltpu.with_memory_space_constraint(x, pltpu.VMEM) for x in sums])
    return gi, gt, loss.reshape(rows)


def solution(mesh):
    placed = (P(("row", "col"), None), P(("row", "col"), None), P(), P())
    return jax.shard_map(
        functools.partial(on_device, mesh.shape["row"], mesh.shape["col"]),
        mesh=mesh,
        in_specs=placed,
        out_specs=(P(("row", "col"), None), P(("row", "col"), None), P(("row", "col"))),
        check_vma=False,
    )
```
